32 devices in a mesh: cuts: 2 (over x), wide: 8 (over z, y), batch: 2 (over core).
Axes of the slice: x: 2, y: 2, z: 4, core: 2. Of those that a mesh axis runs over, the one named last changes fastest.
Arguments:
- initial: bfloat16 [2, 64, 2, 2, 256, 256], P('batch', 'cuts', None, None, None, 'wide'), parts along dimension 1, may hold values from -6 to 6
- branches: bfloat16 [8, 2, 2, 256, 2, 256], P(None, None, None, 'batch'), may hold values from -0.1875 to 0.1875
- projectors: float32 [8, 2, 2, 2], replicated, may hold values from -4 to 4
- bits: int32 [2, 8], P('batch'), may hold values from 0 to 1
Outputs:
- amplitudes: float32 [2, 64, 2, 2, 256, 256], P('batch', 'cuts', None, None, 'wide'), parts along dimension 1
The draws below stay inside these ranges and needn't reach their ends.
There are 2 independent parts, one for each index of `cuts`. The reference program is written for one: setup_inputs(seed, part) draws one part's arguments, and reference() takes and returns one part's arrays. A program takes and returns all parts, laid end to end along the dimension named above; an argument that names none is the same for every part. Nothing has to cross between parts.
Inputs may be any that keep to these rules, and one draw needn't show every extreme that they name: `bits`: each entry is a bit.
All inputs are finite; a program needn't handle non-finite values.
Results may differ from the reference program's by a relative error of at most 0.014.
Values may be sent and summed in bfloat16 or wider, within the bound.
A program may use at most 64 MiB of HBM per device.

```python
import jax
import jax.numpy as jnp

QGROUP = 256
HSHARED = 2
COLUMNS = 32
STEPS = 8
BATCH = 2


def set_ends(values, own_key, least, largest):
    dims = values.shape
    place = [jax.random.randint(jax.random.fold_in(own_key, axis), (), 0, dims[axis]) for axis in range(len(dims))]
    values = values.at[tuple(place)].set(least)
    longest = dims.index(max(dims))
    place[longest] = (place[longest] + 1) % dims[longest]
    return values.at[tuple(place)].set(largest)


def level_of(rng, extent, split, smallest, top_value):
    factor_of, own = 1.0, jax.random.fold_in(rng, 6)
    for dim, shards_of in split:
        steps = jnp.exp(jax.random.uniform(jax.random.fold_in(own, dim), (shards_of,), jnp.float32, smallest / len(split), top_value / len(split)))
        factor_of = factor_of * jnp.repeat(steps, extent[dim] // shards_of).reshape([-1 if axis == dim else 1 for axis in range(len(extent))])
    return factor_of


def scatter_about(rng, dims, deviation, limit, pieces=(), kind=jnp.bfloat16):
    values = jax.random.normal(rng, dims, jnp.float32) * deviation
    if len(pieces) > 0:
        values = level_of(rng, dims, pieces, -0.22, 0.18) * values
    return jnp.clip(values, min=-limit, max=limit).astype(kind)


def setup_inputs(seed: int = 0, part: int = 0) -> dict:
    keys = jax.random.split(jax.random.key(seed), 5)
    part_keys = jax.random.split(jax.random.fold_in(keys[4], part), 5)
    initial = scatter_about(part_keys[0], (BATCH, COLUMNS, 2, HSHARED, QGROUP, QGROUP), 1.0, 6.0, ((0, 2), (5, 8)))
    branches = scatter_about(keys[1], (STEPS, 2, HSHARED, QGROUP, HSHARED, QGROUP), (2 * HSHARED * QGROUP) ** -0.5, 0.1875, ((3, 2),))
    projectors = scatter_about(keys[2], (STEPS, 2, 2, HSHARED), 0.7, 4.0, (), jnp.float32)
    bits = set_ends(jax.random.randint(keys[3], (BATCH, STEPS), 0, 2), jax.random.fold_in(keys[3], 1), 0, 1).astype(jnp.int32)
    return {"initial": initial, "branches": branches, "projectors": projectors, "bits": bits}


def contract(state, branch, select):
    prod = jnp.einsum('ncphuv,thugw->ncptgvw', state.astype(jnp.float32), branch.astype(jnp.float32))
    real_part = prod[:, :, 0, 0] - prod[:, :, 1, 1]
    imag_part = prod[:, :, 0, 1] + prod[:, :, 1, 0]
    proj_re = select[:, 0][:, None, :, None, None]
    proj_im = select[:, 1][:, None, :, None, None]
    out_re = proj_re * real_part - proj_im * imag_part
    out_im = proj_re * imag_part + proj_im * real_part
    return jnp.stack([out_re, out_im], axis=2)


def reference(initial, branches, projectors, bits):
    state = initial
    result = None
    for step in range(STEPS):
        chosen = (bits[:, step] == 1)[:, None, None]
        select = jnp.where(chosen, projectors[step, 1][None], projectors[step, 0][None])
        result = contract(state, branches[step], select)
        state = result.astype(jnp.bfloat16)
    return result
```

```python
import functools

import jax
import jax.numpy as jnp
from jax import lax
from jax.experimental import pallas as pl
from jax.experimental.pallas import tpu as pltpu
from jax.sharding import PartitionSpec as P

MESH = pl.DeviceIdType.MESH
F32 = jnp.float32
BF16 = jnp.bfloat16


def dot(a, b, dims):
    return lax.dot_general(a, b, (dims, ((), ())), preferred_element_type=F32)


def kernel(wide, pair, x_ref, g_ref, proj_ref, bits_ref, out_ref,
           branch, recv1, send2, recv2, state,
           g_send, g_recv, g_local, s1_sem, r1_sem, l1_sem, s2_sem, r2_sem, l2_sem):
    me = lax.axis_index("wide")
    core = lax.axis_index("batch")
    steps = branch.shape[0]
    cols = recv1.shape[0]
    half = g_ref.shape[3]
    group = branch.shape[3]
    vch, width = recv1.shape[4], recv1.shape[5]
    order = sorted(range(1, wide), key=lambda k: (abs(2 * k - wide), k))

    barrier = pltpu.get_barrier_semaphore()
    for k in range(1, wide):
        pl.semaphore_signal(barrier, inc=1, device_id={"wide": lax.rem(me + k, wide)}, device_id_type=MESH)
    for k in range(1, pair):
        pl.semaphore_signal(barrier, inc=1, device_id={"batch": lax.rem(core + k, pair)}, device_id_type=MESH)
    pl.semaphore_wait(barrier, wide + pair - 2)

    def first(j, k):
        peer = lax.rem(me + k, wide)
        return pltpu.make_async_remote_copy(
            x_ref.at[peer, j], recv1.at[j, me], s1_sem.at[j, k], r1_sem.at[j, k],
            device_id={"wide": peer}, device_id_type=MESH)

    def first_own(j):
        return pltpu.make_async_copy(x_ref.at[me, j], recv1.at[j, me], l1_sem.at[j])

    def second(j, k):
        peer = lax.rem(me + k, wide)
        return pltpu.make_async_remote_copy(
            send2.at[j, peer], recv2.at[j, me], s2_sem.at[j, k], r2_sem.at[j, k],
            device_id={"wide": peer}, device_id_type=MESH)

    def second_own(j):
        return pltpu.make_async_copy(send2.at[j, me], recv2.at[j, me], l2_sem.at[j])

    def mine(s):
        return branch.at[s, :, :, pl.ds(pl.multiple_of(core * half, half), half), :]

    def share(s, k):
        return pltpu.make_async_remote_copy(
            g_ref.at[s], mine(s), g_send.at[s, k], g_recv.at[s, k],
            device_id={"batch": lax.rem(core + k, pair)}, device_id_type=MESH)

    def keep(s):
        return pltpu.make_async_copy(g_ref.at[s], mine(s), g_local.at[s])

    def send_column(j, carry):
        for k in order:
            first(j, k).start()
        first_own(j).start()
        return carry

    send_column(0, 0)

    def send_branch(s, carry):
        keep(s).start()
        for k in range(1, pair):
            share(s, k).start()
        return carry

    lax.fori_loop(0, steps, send_branch, 0)
    lax.fori_loop(1, cols, send_column, 0)

    def select(s, g):
        hit = bits_ref[0, s] == 1
        return (jnp.where(hit, proj_ref[s, 4 + g], proj_ref[s, g]),
                jnp.where(hit, proj_ref[s, 6 + g], proj_ref[s, 2 + g]))

    def apply(s, lhs, form, put):
        for g in range(2):
            lanes = pl.ds(g * width, width)
            weight = [branch[s, p, :, :, lanes].reshape(2 * group, width) for p in range(2)]
            if form == "flip":
                prod = [[dot(weight[t], lhs[p], ((0,), (0,))) for t in range(2)] for p in range(2)]
            else:
                axis = 1 if form == "rows" else 0
                prod = [[dot(lhs[p], weight[t], ((axis,), (0,))) for t in range(2)] for p in range(2)]
            re = prod[0][0] - prod[1][1]
            im = prod[0][1] + prod[1][0]
            sr, si = select(s, g)
            put(0, g, sr * re - si * im)
            put(1, g, sr * im + si * re)

    def gathered(buf, j):
        return [jnp.concatenate([buf[j, :, p, h].reshape(wide * vch, width) for h in range(2)], axis=1)
                for p in range(2)]

    def held(slot):
        return [state[slot, p].reshape(2 * group, width) for p in range(2)]

    def column(j, carry):
        for k in order:
            first(j, k).wait_recv()
        first_own(j).wait()

        @pl.when(j == 0)
        def _():
            def arrive(s, carry):
                keep(s).wait()
                for k in range(1, pair):
                    share(s, k).wait_recv()
                return carry
            lax.fori_loop(0, steps, arrive, 0)

        def put_state(slot):
            def put(p, g, value):
                state[slot, p, g] = value.astype(BF16)
            return put

        apply(0, gathered(recv1, j), "rows", put_state(0))

        def middle(s, carry):
            apply(s, held((s + 1) % 2), "columns", put_state(s % 2))
            return carry

        lax.fori_loop(1, steps - 2, middle, 0)

        def put_send(p, g, value):
            send2[j, :, p, g] = value.astype(BF16).reshape(wide, vch, width)

        apply(steps - 2, held((steps - 3) % 2), "flip", put_send)
        for k in order:
            second(j, k).start()
        second_own(j).start()
        return carry

    lax.fori_loop(0, cols, column, 0)

    def last(j, carry):
        for k in order:
            second(j, k).wait_recv()
        second_own(j).wait()

        def put_out(p, g, value):
            out_ref[:, j, p, g] = value.reshape(wide, vch, width)

        apply(steps - 1, gathered(recv2, j), "rows", put_out)
        return carry

    lax.fori_loop(0, cols, last, 0)

    def drain(j, carry):
        for k in order:
            first(j, k).wait_send()
            second(j, k).wait_send()
        return carry

    lax.fori_loop(0, cols, drain, 0)

    def drain_branch(s, carry):
        for k in range(1, pair):
            share(s, k).wait_send()
        return carry

    lax.fori_loop(0, steps, drain_branch, 0)


def solution(mesh):
    wide, pair = mesh.shape["wide"], mesh.shape["batch"]

    def shards(initial, branches, projectors, bits):
        _, columns, parts, shared, group, vch = initial.shape
        steps, half, width = branches.shape[0], branches.shape[3], branches.shape[5]
        cols = columns // wide
        x = jnp.swapaxes(initial, 4, 5).reshape(wide, cols, parts, shared, vch, group)
        g = branches.reshape(steps, parts, shared, half, shared * width)
        proj = projectors.reshape(steps, -1)
        dma = pltpu.SemaphoreType.DMA
        chunk = (cols, wide, parts, shared, vch, width)
        out = pl.pallas_call(
            functools.partial(kernel, wide, pair),
            out_shape=jax.ShapeDtypeStruct((wide, cols, parts, shared, vch, width), F32),
            in_specs=[
                pl.BlockSpec(memory_space=pl.ANY),
                pl.BlockSpec(memory_space=pl.ANY),
                pl.BlockSpec(memory_space=pltpu.SMEM),
                pl.BlockSpec(memory_space=pltpu.SMEM),
            ],
            out_specs=pl.BlockSpec(memory_space=pltpu.VMEM),
            scratch_shapes=[
                pltpu.VMEM((steps, parts, shared, half * pair, shared * width), BF16),
                pltpu.VMEM(chunk, BF16),
                pltpu.VMEM(chunk, BF16),
                pltpu.VMEM(chunk, BF16),
                pltpu.VMEM((2, parts, shared, group, width), BF16),
                dma((steps, pair)), dma((steps, pair)), dma((steps,)),
                dma((cols, wide)), dma((cols, wide)), dma((cols,)),
                dma((cols, wide)), dma((cols, wide)), dma((cols,)),
            ],
            compiler_params=pltpu.CompilerParams(
                collective_id=0, has_side_effects=True, vmem_limit_bytes=48 * 1024 * 1024),
        )(x, g, proj, bits)
        return out.reshape(1, columns, parts, shared, vch, width)

    in_specs = (
        P("batch", "cuts", None, None, None, "wide"),
        P(None, None, None, "batch", None, None),
        P(),
        P("batch", None),
    )
    out_specs = P("batch", "cuts", None, None, "wide", None)
    return jax.shard_map(shards, mesh=mesh, in_specs=in_specs, out_specs=out_specs, check_vma=False)
```

```python
import functools

import jax
import jax.numpy as jnp
from jax import lax
from jax.experimental import pallas as pl
from jax.experimental.pallas import tpu as pltpu
from jax.sharding import PartitionSpec as P

MESH = pl.DeviceIdType.MESH
F32 = jnp.float32
BF16 = jnp.bfloat16


def dot(a, b, dims):
    return lax.dot_general(a, b, (dims, ((), ())), preferred_element_type=F32)


def kernel(wide, pair, x_ref, g_ref, proj_ref, bits_ref, out_ref,
           branch, recv1, send2, recv2, state, result, out_sem,
           g_send, g_recv, g_local, s1_sem, r1_sem, l1_sem, s2_sem, r2_sem, l2_sem):
    me = lax.axis_index("wide")
    core = lax.axis_index("batch")
    steps = branch.shape[0]
    cols = recv1.shape[0]
    half = g_ref.shape[4]
    group = branch.shape[4]
    vch, width = recv1.shape[4], recv1.shape[5]
    order = sorted(range(1, wide), key=lambda k: (abs(2 * k - wide), k))

    barrier = pltpu.get_barrier_semaphore()
    for k in range(1, wide):
        pl.semaphore_signal(barrier, inc=1, device_id={"wide": lax.rem(me + k, wide)}, device_id_type=MESH)
    for k in range(1, pair):
        pl.semaphore_signal(barrier, inc=1, device_id={"batch": lax.rem(core + k, pair)}, device_id_type=MESH)
    pl.semaphore_wait(barrier, wide + pair - 2)

    def first(j, k):
        peer = lax.rem(me + k, wide)
        return pltpu.make_async_remote_copy(
            x_ref.at[peer, j], recv1.at[j, me], s1_sem.at[j, k], r1_sem.at[j, k],
            device_id={"wide": peer}, device_id_type=MESH)

    def first_own(j):
        return pltpu.make_async_copy(x_ref.at[me, j], recv1.at[j, me], l1_sem.at[j])

    def second(j, k):
        peer = lax.rem(me + k, wide)
        return pltpu.make_async_remote_copy(
            send2.at[j, peer], recv2.at[j, me], s2_sem.at[j, k], r2_sem.at[j, k],
            device_id={"wide": peer}, device_id_type=MESH)

    def second_own(j):
        return pltpu.make_async_copy(send2.at[j, me], recv2.at[j, me], l2_sem.at[j])

    def mine(s):
        return branch.at[s, :, :, :, pl.ds(pl.multiple_of(core * half, half), half), :]

    def share(s, k):
        return pltpu.make_async_remote_copy(
            g_ref.at[s], mine(s), g_send.at[s, k], g_recv.at[s, k],
            device_id={"batch": lax.rem(core + k, pair)}, device_id_type=MESH)

    def keep(s):
        return pltpu.make_async_copy(g_ref.at[s], mine(s), g_local.at[s])

    def send_column(j, carry):
        for k in order:
            first(j, k).start()
        first_own(j).start()
        return carry

    send_column(0, 0)

    def send_branch(s, carry):
        keep(s).start()
        for k in range(1, pair):
            share(s, k).start()
        return carry

    lax.fori_loop(0, steps, send_branch, 0)
    lax.fori_loop(1, cols, send_column, 0)

    def select(s, g):
        hit = bits_ref[0, s] == 1
        return (jnp.where(hit, proj_ref[s, 4 + g], proj_ref[s, g]),
                jnp.where(hit, proj_ref[s, 6 + g], proj_ref[s, 2 + g]))

    def apply(s, lhs, form, put):
        for g in range(2):
            weight = [branch[s, p, g].reshape(2 * group, width) for p in range(2)]
            if form == "flip":
                prod = [[dot(weight[t], lhs[p], ((0,), (0,))) for t in range(2)] for p in range(2)]
            else:
                axis = 1 if form == "rows" else 0
                prod = [[dot(lhs[p], weight[t], ((axis,), (0,))) for t in range(2)] for p in range(2)]
            re = prod[0][0] - prod[1][1]
            im = prod[0][1] + prod[1][0]
            sr, si = select(s, g)
            put(0, g, sr * re - si * im)
            put(1, g, sr * im + si * re)

    def gathered(buf, j):
        return [jnp.concatenate([buf[j, :, p, h].reshape(wide * vch, width) for h in range(2)], axis=1)
                for p in range(2)]

    def held(slot):
        return [state[slot, p].reshape(2 * group, width) for p in range(2)]

    def column(j, carry):
        for k in order:
            first(j, k).wait_recv()
        first_own(j).wait()

        @pl.when(j == 0)
        def _():
            def arrive(s, carry):
                keep(s).wait()
                for k in range(1, pair):
                    share(s, k).wait_recv()
                return carry
            lax.fori_loop(0, steps, arrive, 0)

        def put_state(slot):
            def put(p, g, value):
                state[slot, p, g] = value.astype(BF16)
            return put

        apply(0, gathered(recv1, j), "rows", put_state(0))

        def middle(s, carry):
            apply(s, held((s + 1) % 2), "columns", put_state(s % 2))
            return carry

        lax.fori_loop(1, steps - 2, middle, 0)

        def put_send(p, g, value):
            send2[j, :, p, g] = value.astype(BF16).reshape(wide, vch, width)

        apply(steps - 2, held((steps - 3) % 2), "flip", put_send)
        for k in order:
            second(j, k).start()
        second_own(j).start()
        return carry

    lax.fori_loop(0, cols, column, 0)

    def leave(j):
        return pltpu.make_async_copy(result.at[:, j], out_ref.at[:, j], out_sem.at[j])

    def last(j, carry):
        for k in order:
            second(j, k).wait_recv()
        second_own(j).wait()

        def put_out(p, g, value):
            result[:, j, p, g] = value.reshape(wide, vch, width)

        apply(steps - 1, gathered(recv2, j), "rows", put_out)
        leave(j).start()
        return carry

    lax.fori_loop(0, cols, last, 0)

    def drain(j, carry):
        for k in order:
            first(j, k).wait_send()
            second(j, k).wait_send()
        leave(j).wait()
        return carry

    lax.fori_loop(0, cols, drain, 0)

    def drain_branch(s, carry):
        for k in range(1, pair):
            share(s, k).wait_send()
        return carry

    lax.fori_loop(0, steps, drain_branch, 0)


def solution(mesh):
    wide, pair = mesh.shape["wide"], mesh.shape["batch"]

    def shards(initial, branches, projectors, bits):
        _, columns, parts, shared, group, vch = initial.shape
        steps, half, width = branches.shape[0], branches.shape[3], branches.shape[5]
        cols = columns // wide
        x = jnp.swapaxes(initial, 4, 5).reshape(wide, cols, parts, shared, vch, group)
        g = jnp.transpose(branches, (0, 1, 4, 2, 3, 5))
        proj = projectors.reshape(steps, -1)
        dma = pltpu.SemaphoreType.DMA
        chunk = (cols, wide, parts, shared, vch, width)
        chunk_out = (wide, cols, parts, shared, vch, width)
        out = pl.pallas_call(
            functools.partial(kernel, wide, pair),
            out_shape=jax.ShapeDtypeStruct(chunk_out, F32),
            in_specs=[
                pl.BlockSpec(memory_space=pl.ANY),
                pl.BlockSpec(memory_space=pl.ANY),
                pl.BlockSpec(memory_space=pltpu.SMEM),
                pl.BlockSpec(memory_space=pltpu.SMEM),
            ],
            out_specs=pl.BlockSpec(memory_space=pl.ANY),
            scratch_shapes=[
                pltpu.VMEM((steps, parts, shared, shared, half * pair, width), BF16),
                pltpu.VMEM(chunk, BF16),
                pltpu.VMEM(chunk, BF16),
                pltpu.VMEM(chunk, BF16),
                pltpu.VMEM((2, parts, shared, group, width), BF16),
                pltpu.VMEM(chunk_out, F32),
                dma((cols,)),
                dma((steps, pair)), dma((steps, pair)), dma((steps,)),
                dma((cols, wide)), dma((cols, wide)), dma((cols,)),
                dma((cols, wide)), dma((cols, wide)), dma((cols,)),
            ],
            compiler_params=pltpu.CompilerParams(
                collective_id=0, has_side_effects=True, vmem_limit_bytes=32 * 1024 * 1024),
        )(x, g, proj, bits)
        return out.reshape(1, columns, parts, shared, vch, width)

    in_specs = (
        P("batch", "cuts", None, None, None, "wide"),
        P(None, None, None, "batch", None, None),
        P(),
        P("batch", None),
    )
    out_specs = P("batch", "cuts", None, None, "wide", None)
    return jax.shard_map(shards, mesh=mesh, in_specs=in_specs, out_specs=out_specs, check_vma=False)
```

```python
import functools

import jax
import jax.numpy as jnp
from jax import lax
from jax.experimental import pallas as pl
from jax.experimental.pallas import tpu as pltpu
from jax.sharding import PartitionSpec as P

MESH = pl.DeviceIdType.MESH
F32 = jnp.float32
BF16 = jnp.bfloat16


def dot(a, b, dims):
    return lax.dot_general(a, b, (dims, ((), ())), preferred_element_type=F32)


def kernel(wide, pair, x_ref, g_ref, proj_ref, bits_ref, out_ref,
           raw, branch, recv1, send2, recv2, state, result, out_sem,
           g_send, g_recv, g_local, s1_sem, r1_sem, l1_sem, s2_sem, r2_sem, l2_sem):
    me = lax.axis_index("wide")
    core = lax.axis_index("batch")
    steps = branch.shape[0]
    cols = recv1.shape[0]
    half = g_ref.shape[3]
    group = branch.shape[4]
    vch, width = recv1.shape[4], recv1.shape[5]
    near = range(1, wide)
    far = sorted(near, key=lambda k: -k.bit_length())

    def partner(k):
        peer, bit = 0, 1
        while bit < wide:
            digit = lax.rem(me // bit, 2)
            peer = peer + bit * (1 - digit if (k // bit) % 2 else digit)
            bit *= 2
        return peer

    barrier = pltpu.get_barrier_semaphore()
    for k in range(1, wide):
        pl.semaphore_signal(barrier, inc=1, device_id={"wide": partner(k)}, device_id_type=MESH)
    for k in range(1, pair):
        pl.semaphore_signal(barrier, inc=1, device_id={"batch": lax.rem(core + k, pair)}, device_id_type=MESH)
    pl.semaphore_wait(barrier, wide + pair - 2)

    def first(j, k):
        peer = partner(k)
        return pltpu.make_async_remote_copy(
            x_ref.at[peer, j], recv1.at[j, me], s1_sem.at[j, k], r1_sem.at[j, k],
            device_id={"wide": peer}, device_id_type=MESH)

    def first_own(j):
        return pltpu.make_async_copy(x_ref.at[me, j], recv1.at[j, me], l1_sem.at[j])

    def second(j, k):
        peer = partner(k)
        return pltpu.make_async_remote_copy(
            send2.at[j, peer], recv2.at[j, me], s2_sem.at[j, k], r2_sem.at[j, k],
            device_id={"wide": peer}, device_id_type=MESH)

    def second_own(j):
        return pltpu.make_async_copy(send2.at[j, me], recv2.at[j, me], l2_sem.at[j])

    def mine(s):
        return raw.at[s, :, :, pl.ds(pl.multiple_of(core * half, half), half)]

    def share(s, k):
        return pltpu.make_async_remote_copy(
            g_ref.at[s], mine(s), g_send.at[s, k], g_recv.at[s, k],
            device_id={"batch": lax.rem(core + k, pair)}, device_id_type=MESH)

    def keep(s):
        return pltpu.make_async_copy(g_ref.at[s], mine(s), g_local.at[s])

    def send_column(j, carry):
        first_own(j).start()
        for k in near:
            first(j, k).start()
        return carry

    for k in far:
        first(0, k).start()
    first_own(0).start()

    def send_branch(s, carry):
        keep(s).start()
        for k in range(1, pair):
            share(s, k).start()
        return carry

    lax.fori_loop(0, steps, send_branch, 0)
    lax.fori_loop(1, cols, send_column, 0)

    def arrive(s, carry):
        keep(s).wait()
        for k in range(1, pair):
            share(s, k).wait_recv()
        for p in range(2):
            for h in range(2):
                both = raw[s, p, h]
                for g in range(2):
                    branch[s, p, g, h] = both[:, g, :]
        return carry
    lax.fori_loop(0, steps, arrive, 0)

    def select(s, g):
        hit = bits_ref[0, s] == 1
        return (jnp.where(hit, proj_ref[4 + g, s], proj_ref[g, s]),
                jnp.where(hit, proj_ref[6 + g, s], proj_ref[2 + g, s]))

    def apply(s, lhs, form, put):
        for g in range(2):
            weight = [branch[s, p, g].reshape(2 * group, width) for p in range(2)]
            if form == "flip":
                prod = [[dot(weight[t], lhs[p], ((0,), (0,))) for t in range(2)] for p in range(2)]
            else:
                axis = 1 if form == "rows" else 0
                prod = [[dot(lhs[p], weight[t], ((axis,), (0,))) for t in range(2)] for p in range(2)]
            re = prod[0][0] - prod[1][1]
            im = prod[0][1] + prod[1][0]
            sr, si = select(s, g)
            put(0, g, sr * re - si * im)
            put(1, g, sr * im + si * re)

    def gathered(buf, j):
        return [jnp.concatenate([buf[j, :, p, h].reshape(wide * vch, width) for h in range(2)], axis=1)
                for p in range(2)]

    def held(slot):
        return [state[slot, p].reshape(2 * group, width) for p in range(2)]

    def column(j, carry):
        for k in near:
            first(j, k).wait_recv()
        first_own(j).wait()

        def put_state(slot):
            def put(p, g, value):
                state[slot, p, g] = value.astype(BF16)
            return put

        apply(0, gathered(recv1, j), "rows", put_state(0))

        def middle(s, carry):
            apply(s, held((s + 1) % 2), "columns", put_state(s % 2))
            return carry

        lax.fori_loop(1, steps - 2, middle, 0)

        def put_send(p, g, value):
            send2[j, :, p, g] = value.astype(BF16).reshape(wide, vch, width)

        apply(steps - 2, held((steps - 3) % 2), "flip", put_send)
        for k in near:
            second(j, k).start()
        second_own(j).start()
        return carry

    lax.fori_loop(0, cols, column, 0)

    def leave(j):
        return pltpu.make_async_copy(result.at[:, j], out_ref.at[:, j], out_sem.at[j])

    def last(j, carry):
        for k in near:
            second(j, k).wait_recv()
        second_own(j).wait()

        def put_out(p, g, value):
            result[:, j, p, g] = value.reshape(wide, vch, width)

        apply(steps - 1, gathered(recv2, j), "rows", put_out)
        leave(j).start()
        return carry

    lax.fori_loop(0, cols, last, 0)

    def drain(j, carry):
        for k in near:
            first(j, k).wait_send()
            second(j, k).wait_send()
        leave(j).wait()
        return carry

    lax.fori_loop(0, cols, drain, 0)

    def drain_branch(s, carry):
        for k in range(1, pair):
            share(s, k).wait_send()
        return carry

    lax.fori_loop(0, steps, drain_branch, 0)


def solution(mesh):
    wide, pair = mesh.shape["wide"], mesh.shape["batch"]

    def shards(initial, branches, projectors, bits):
        _, columns, parts, shared, group, vch = initial.shape
        steps, half, width = branches.shape[0], branches.shape[3], branches.shape[5]
        cols = columns // wide
        x = jnp.swapaxes(initial, 4, 5).reshape(wide, cols, parts, shared, vch, group)
        proj = jnp.transpose(projectors, (1, 2, 3, 0)).reshape(-1, steps)
        dma = pltpu.SemaphoreType.DMA
        chunk = (cols, wide, parts, shared, vch, width)
        chunk_out = (wide, cols, parts, shared, vch, width)
        out = pl.pallas_call(
            functools.partial(kernel, wide, pair),
            out_shape=jax.ShapeDtypeStruct(chunk_out, F32),
            in_specs=[
                pl.BlockSpec(memory_space=pltpu.HBM),
                pl.BlockSpec(memory_space=pltpu.HBM),
                pl.BlockSpec(memory_space=pltpu.SMEM),
                pl.BlockSpec(memory_space=pltpu.SMEM),
            ],
            out_specs=pl.BlockSpec(memory_space=pl.ANY),
            scratch_shapes=[
                pltpu.VMEM((steps, parts, shared, half * pair, shared, width), BF16),
                pltpu.VMEM((steps, parts, shared, shared, half * pair, width), BF16),
                pltpu.VMEM(chunk, BF16),
                pltpu.VMEM(chunk, BF16),
                pltpu.VMEM(chunk, BF16),
                pltpu.VMEM((2, parts, shared, group, width), BF16),
                pltpu.VMEM(chunk_out, F32),
                dma((cols,)),
                dma((steps, pair)), dma((steps, pair)), dma((steps,)),
                dma((cols, wide)), dma((cols, wide)), dma((cols,)),
                dma((cols, wide)), dma((cols, wide)), dma((cols,)),
            ],
            compiler_params=pltpu.CompilerParams(
                collective_id=0, has_side_effects=True, vmem_limit_bytes=32 * 1024 * 1024),
        )(x, branches, proj, bits)
        return out.reshape(1, columns, parts, shared, vch, width)

    in_specs = (
        P("batch", "cuts", None, None, None, "wide"),
        P(None, None, None, "batch", None, None),
        P(),
        P("batch", None),
    )
    out_specs = P("batch", "cuts", None, None, "wide", None)
    return jax.shard_map(shards, mesh=mesh, in_specs=in_specs, out_specs=out_specs, check_vma=False)
```

```python
import functools

import jax
import jax.numpy as jnp
from jax import lax
from jax.experimental import pallas as pl
from jax.experimental.pallas import tpu as pltpu
from jax.sharding import PartitionSpec as P

MESH = pl.DeviceIdType.MESH
F32 = jnp.float32
BF16 = jnp.bfloat16


def dot(a, b, dims):
    return lax.dot_general(a, b, (dims, ((), ())), preferred_element_type=F32)


def kernel(wide, pair, x_ref, g_ref, proj_ref, bits_ref, out_ref,
           raw, branch, recv1, send2, recv2, state, result, out_sem,
           g_send, g_recv, g_local, s1_sem, r1_sem, l1_sem, s2_sem, r2_sem, l2_sem):
    me = lax.axis_index("wide")
    core = lax.axis_index("batch")
    steps = branch.shape[0]
    cols = recv1.shape[0]
    half = g_ref.shape[3]
    group = branch.shape[4]
    vch, width = recv1.shape[4], recv1.shape[5]
    near = range(1, wide)
    far = sorted(near, key=lambda k: -k.bit_length())

    def partner(k):
        peer, bit = 0, 1
        while bit < wide:
            digit = lax.rem(me // bit, 2)
            peer = peer + bit * (1 - digit if (k // bit) % 2 else digit)
            bit *= 2
        return peer

    barrier = pltpu.get_barrier_semaphore()
    for k in range(1, wide):
        pl.semaphore_signal(barrier, inc=1, device_id={"wide": partner(k)}, device_id_type=MESH)
    for k in range(1, pair):
        pl.semaphore_signal(barrier, inc=1, device_id={"batch": lax.rem(core + k, pair)}, device_id_type=MESH)
    pl.semaphore_wait(barrier, wide + pair - 2)

    def first(j, k):
        peer = partner(k)
        return pltpu.make_async_remote_copy(
            x_ref.at[peer, j], recv1.at[j, me], s1_sem.at[j, k], r1_sem.at[j, k],
            device_id={"wide": peer}, device_id_type=MESH)

    def first_own(j):
        return pltpu.make_async_copy(x_ref.at[me, j], recv1.at[j, me], l1_sem.at[j])

    def second(j, k):
        peer = partner(k)
        return pltpu.make_async_remote_copy(
            send2.at[j, peer], recv2.at[j, me], s2_sem.at[j, k], r2_sem.at[j, k],
            device_id={"wide": peer}, device_id_type=MESH)

    def second_own(j):
        return pltpu.make_async_copy(send2.at[j, me], recv2.at[j, me], l2_sem.at[j])

    def mine(s):
        return raw.at[s, :, :, pl.ds(pl.multiple_of(core * half, half), half)]

    def share(s, k):
        return pltpu.make_async_remote_copy(
            g_ref.at[s], mine(s), g_send.at[s, k], g_recv.at[s, k],
            device_id={"batch": lax.rem(core + k, pair)}, device_id_type=MESH)

    def keep(s):
        return pltpu.make_async_copy(g_ref.at[s], mine(s), g_local.at[s])

    def send_column(j, carry):
        first_own(j).start()
        for k in near:
            first(j, k).start()
        return carry

    for k in far:
        first(0, k).start()
    first_own(0).start()

    def send_branch(s, carry):
        keep(s).start()
        for k in range(1, pair):
            share(s, k).start()
        return carry

    lax.fori_loop(0, steps, send_branch, 0)
    lax.fori_loop(1, cols, send_column, 0)

    def arrive(s, carry):
        keep(s).wait()
        for k in range(1, pair):
            share(s, k).wait_recv()
        for p in range(2):
            for h in range(2):
                both = raw[s, p, h]
                for g in range(2):
                    branch[s, p, g, h] = both[:, g, :]
        return carry
    lax.fori_loop(0, steps, arrive, 0)

    def select(s, g):
        hit = bits_ref[0, s] == 1
        return (jnp.where(hit, proj_ref[4 + g, s], proj_ref[g, s]),
                jnp.where(hit, proj_ref[6 + g, s], proj_ref[2 + g, s]))

    def apply(s, lhs, form, put):
        for g in range(2):
            weight = [branch[s, p, g].reshape(2 * group, width) for p in range(2)]
            if form == "flip":
                prod = [[dot(weight[t], lhs[p], ((0,), (0,))) for t in range(2)] for p in range(2)]
            else:
                axis = 1 if form == "rows" else 0
                prod = [[dot(lhs[p], weight[t], ((axis,), (0,))) for t in range(2)] for p in range(2)]
            re = prod[0][0] - prod[1][1]
            im = prod[0][1] + prod[1][0]
            sr, si = select(s, g)
            put(0, g, sr * re - si * im)
            put(1, g, sr * im + si * re)

    def gathered(buf, j):
        return [jnp.concatenate([buf[j, :, p, h].reshape(wide * vch, width) for h in range(2)], axis=1)
                for p in range(2)]

    def held(slot):
        return [state[slot, p].reshape(2 * group, width) for p in range(2)]

    def column(j, carry):
        for k in near:
            first(j, k).wait_recv()
        first_own(j).wait()

        def put_state(slot):
            def put(p, g, value):
                state[slot, p, g] = value.astype(BF16)
            return put

        apply(0, gathered(recv1, j), "rows", put_state(0))

        def middle(s, carry):
            apply(s, held((s + 1) % 2), "columns", put_state(s % 2))
            return carry

        lax.fori_loop(1, steps - 2, middle, 0)

        def put_send(p, g, value):
            send2[j, :, p, g] = value.astype(BF16).reshape(wide, vch, width)

        apply(steps - 2, held((steps - 3) % 2), "flip", put_send)
        for k in near:
            second(j, k).start()
        second_own(j).start()
        return carry

    lax.fori_loop(0, cols, column, 0)

    def leave(j):
        return pltpu.make_async_copy(result.at[:, j], out_ref.at[:, j], out_sem.at[j])

    def last(j, carry):
        for k in near:
            second(j, k).wait_recv()
        second_own(j).wait()

        def put_out(p, g, value):
            result[:, j, p, g] = value.reshape(wide, vch, width)

        apply(steps - 1, gathered(recv2, j), "rows", put_out)
        leave(j).start()
        return carry

    lax.fori_loop(0, cols, last, 0)

    def drain(j, carry):
        for k in near:
            first(j, k).wait_send()
            second(j, k).wait_send()
        leave(j).wait()
        return carry

    lax.fori_loop(0, cols, drain, 0)

    def drain_branch(s, carry):
        for k in range(1, pair):
            share(s, k).wait_send()
        return carry

    lax.fori_loop(0, steps, drain_branch, 0)


def solution(mesh):
    wide, pair = mesh.shape["wide"], mesh.shape["batch"]

    def shards(initial, branches, projectors, bits):
        _, columns, parts, shared, group, vch = initial.shape
        steps, half, width = branches.shape[0], branches.shape[3], branches.shape[5]
        cols = columns // wide
        x = jnp.swapaxes(initial, 4, 5).reshape(wide, cols, parts, shared, vch, group)
        proj = jnp.transpose(projectors, (1, 2, 3, 0)).reshape(-1, steps)
        dma = pltpu.SemaphoreType.DMA
        chunk = (cols, wide, parts, shared, vch, width)
        chunk_out = (wide, cols, parts, shared, vch, width)
        out = pl.pallas_call(
            functools.partial(kernel, wide, pair),
            out_shape=jax.ShapeDtypeStruct(chunk_out, F32),
            in_specs=[
                pl.BlockSpec(memory_space=pltpu.HBM),
                pl.BlockSpec(memory_space=pltpu.HBM),
                pl.BlockSpec(memory_space=pltpu.SMEM),
                pl.BlockSpec(memory_space=pltpu.SMEM),
            ],
            out_specs=pl.BlockSpec(memory_space=pl.ANY),
            scratch_shapes=[
                pltpu.VMEM((steps, parts, shared, half * pair, shared, width), BF16),
                pltpu.VMEM((steps, parts, shared, shared, half * pair, width), BF16),
                pltpu.VMEM(chunk, BF16),
                pltpu.VMEM(chunk, BF16),
                pltpu.VMEM(chunk, BF16),
                pltpu.VMEM((2, parts, shared, group, width), BF16),
                pltpu.VMEM(chunk_out, F32),
                dma((cols,)),
                dma((steps, pair)), dma((steps, pair)), dma((steps,)),
                dma((cols, wide)), dma((cols, wide)), dma((cols,)),
                dma((cols, wide)), dma((cols, wide)), dma((cols,)),
            ],
            compiler_params=pltpu.CompilerParams(
                collective_id=0, has_side_effects=True, vmem_limit_bytes=44 * 1024 * 1024),
        )(x, branches, proj, bits)
        return out.reshape(1, columns, parts, shared, vch, width)

    in_specs = (
        P("batch", "cuts", None, None, None, "wide"),
        P(None, None, None, "batch", None, None),
        P(),
        P("batch", None),
    )
    out_specs = P("batch", "cuts", None, None, "wide", None)
    return jax.shard_map(shards, mesh=mesh, in_specs=in_specs, out_specs=out_specs, check_vma=False)
```
